32 devices in a mesh: seq: 8 (over z, y), mp: 4 (over x, core).
Axes of the slice: x: 2, y: 2, z: 4, core: 2. Of those that a mesh axis runs over, the one named last changes fastest.
Arguments:
- gate_in: bfloat16 [8192, 1024], P('seq', 'mp'), may hold values from -5 to 5
- value_in: bfloat16 [8192, 1024], P('seq', 'mp'), may hold values from -5 to 5
- out_gate: bfloat16 [8192, 1024], P('seq', 'mp'), may hold values from -10 to 10
- filter_taps: bfloat16 [4096, 1024], P('seq', 'mp'), may hold values from -0.09375 to 0.09375
- skip_gain: float32 [1024], P('mp'), may hold values from -4 to 4
Outputs:
- output: bfloat16 [8192, 1024], P('seq', 'mp')
The draws below stay inside these ranges and needn't reach their ends.
All inputs are finite; a program needn't handle non-finite values.
Results may differ from the reference program's by a relative error of at most 0.009.
Values may be sent and summed in bfloat16 or wider, within the bound.
A program may use at most 64 MiB of HBM per device.

```python
import math
import jax
import jax.numpy as jnp
from jax import lax

C = 1024
K = 4096
TOKENS = 8192


def draw_out_gate(key, part):
    first_key, second_key = jax.random.split(jax.random.fold_in(key, 11), 2)
    position = jnp.arange(C, dtype=jnp.float32) / (C - 1)
    ramp = 0.55 * jnp.power(3.0, position)
    channel_scale = jnp.exp(jax.random.uniform(second_key, (C,), jnp.float32, math.log(0.7), math.log(1.4)))
    base = jnp.clip(jax.random.normal(first_key, (TOKENS, C), jnp.float32), -4.0, 4.0)
    return (base * ramp[None, :] * channel_scale[None, :]).astype(jnp.bfloat16)


def block_scale(key, dims, pieces, smallest, largest):
    def one(dim, parts):
        draws = jax.random.uniform(jax.random.fold_in(jax.random.fold_in(key, 6), dim), (parts,), jnp.float32, smallest / len(pieces), largest / len(pieces))
        return jnp.repeat(jnp.exp(draws), dims[dim] // parts).reshape((-1,) + (1,) * (len(dims) - dim - 1))

    loudness = one(*pieces[0])
    for cut in pieces[1:]:
        loudness = loudness * one(*cut)
    return loudness


def gaussian(stream_key, extent, scale, bound, cuts=(), held_as=jnp.bfloat16):
    loudness = block_scale(stream_key, extent, cuts, -0.22, 0.18) if cuts else 1.0
    entries = jax.random.normal(stream_key, extent, jnp.float32) * scale * loudness
    return jnp.minimum(jnp.maximum(entries, -bound), bound).astype(held_as)


def setup_inputs(seed: int = 0) -> dict:
    keys = jax.random.split(jax.random.key(seed), 6)
    return {
        "gate_in": gaussian(keys[0], (TOKENS, C), 1.0, 5.0, ((0, 8), (1, 4))),
        "value_in": gaussian(keys[1], (TOKENS, C), 1.0, 5.0, ((0, 8), (1, 4))),
        "out_gate": draw_out_gate(jax.random.fold_in(keys[5], 71), 0),
        "filter_taps": gaussian(keys[3], (K, C), K ** -0.5, 0.09375, ((0, 8), (1, 4))),
        "skip_gain": gaussian(keys[4], (C,), 1.0, 4.0, ((0, 4),), jnp.float32),
    }


def convolve_group(signal_kernel):
    signal, kernel = signal_kernel
    length = signal.shape[1]
    size = 1 << (length + kernel.shape[1] - 1).bit_length()
    product = jnp.fft.rfft(signal, size) * jnp.fft.rfft(kernel, size)
    return jnp.fft.irfft(product, size)[:, :length]

def reference(gate_in, value_in, out_gate, filter_taps, skip_gain):
    gated = (gate_in.astype(jnp.float32) * value_in.astype(jnp.float32)).astype(jnp.bfloat16)
    group = 32
    signal = gated.astype(jnp.float32).T.reshape(C // group, group, TOKENS)
    kernel = filter_taps.astype(jnp.float32).T.reshape(C // group, group, K)
    convolved = lax.map(convolve_group, (signal, kernel)).reshape(C, TOKENS).T
    mixed = out_gate.astype(jnp.float32) * (convolved + skip_gain[None, :] * gated.astype(jnp.float32))
    power = lax.optimization_barrier(jnp.mean(mixed * mixed, axis=1, keepdims=True))
    return (mixed / jnp.sqrt(power + 1e-05)).astype(jnp.bfloat16)
```

```python
import functools

import jax
import jax.numpy as jnp
from jax import lax
from jax.experimental import pallas as pl
from jax.experimental.pallas import tpu as pltpu
from jax.sharding import PartitionSpec as P

MESH = pl.DeviceIdType.MESH
LANES = 128
TAPS, GATED, RESULT = 0, 1, 2
EPS = 1e-05


def forward_peer(me, i, n):
    if n & (n - 1) == 0:
        return me ^ (n - 1 - i)
    return lax.rem(me + 1 + i, n)


def result_peer(me, i, n):
    if n & (n - 1) or n < 4:
        return lax.rem(me + 1 + i, n)
    odd = lax.rem(me, 2)
    return jnp.where(i < me - odd, i, i + 1) ^ odd


def mp_peer(mine, k, m):
    return lax.rem(mine + k, m)


def kernel(cfg, gate_in, value_in, og_in, taps_in, skip_in, mixed, sums, gate, value, og, taps, skip, stage_h,
           stage_x, xm, hm, xr, hr, hf, xpad, rs, cr, ogt, power, powers, load_sem, send_sem, recv_sem,
           own_sem, psend_sem, precv_sem):
    n, m, channels, blocks, cl, width, groups, phases, sent_taps, hs, he, total_c = cfg
    me = lax.axis_index("seq")
    mine = lax.axis_index("mp")
    nd = hs * he
    pc = channels // phases
    per_phase = groups // phases

    def load(i, p):
        src, dst = [(taps_in, taps), (gate_in, gate), (value_in, value)][i]
        cols = slice(p * pc, (p + 1) * pc)
        return pltpu.make_async_copy(src.at[:, cols], dst.at[:, cols], load_sem.at[i, p])

    og_load = pltpu.make_async_copy(og_in, og, load_sem.at[3, 0])
    skip_load = pltpu.make_async_copy(skip_in, skip, load_sem.at[4, 0])
    for p in range(phases):
        for i in ([0, 1, 2] if sent_taps else [1, 2]):
            load(i, p).start()
    if not sent_taps:
        whole_taps = pltpu.make_async_copy(taps_in, taps, load_sem.at[0, 0])
        whole_taps.start()

    barrier = pltpu.get_barrier_semaphore()
    for i in range(n - 1):
        pl.semaphore_signal(barrier, inc=1, device_id={"seq": forward_peer(me, i, n)}, device_id_type=MESH)
    for k in range(1, m):
        pl.semaphore_signal(barrier, inc=1, device_id={"mp": mp_peer(mine, k, m)}, device_id_type=MESH)
    og_load.start()
    skip_load.start()

    def rows_of(kind, g):
        per = he if kind == TAPS else blocks
        return pl.ds(g * width * per, width * per)

    def refs(kind):
        return {TAPS: (hm, hr), GATED: (xm, xr), RESULT: (rs, cr)}[kind]

    def remote(kind, g, to):
        src, dst = refs(kind)
        rows = rows_of(kind, g)
        return pltpu.make_async_remote_copy(
            src_ref=src.at[to, rows],
            dst_ref=dst.at[me, rows],
            send_sem=send_sem.at[kind, g, to],
            recv_sem=recv_sem.at[kind, g, me],
            device_id={"seq": to},
            device_id_type=MESH,
        )

    def arrival(kind, g, whence):
        src, dst = refs(kind)
        rows = rows_of(kind, g)
        return pltpu.make_async_remote_copy(
            src_ref=src.at[whence, rows],
            dst_ref=dst.at[whence, rows],
            send_sem=send_sem.at[kind, g, whence],
            recv_sem=recv_sem.at[kind, g, whence],
            device_id={"seq": whence},
            device_id_type=MESH,
        )

    def own(kind, g):
        src, dst = refs(kind)
        rows = rows_of(kind, g)
        return pltpu.make_async_copy(src.at[me, rows], dst.at[me, rows], own_sem.at[kind, g])

    def peer(kind, i):
        return result_peer(me, i, n) if kind == RESULT else forward_peer(me, i, n)

    forward = ([TAPS] if sent_taps else []) + [GATED]

    def put(stage, dst, p, per):
        for q in range(per_phase):
            g = p * per_phase + q
            size = n * width * per
            part = stage[q * size:(q + 1) * size, :].astype(jnp.bfloat16)
            dst[:, g * width * per:(g + 1) * width * per, :] = part.reshape(n, width * per, LANES)

    for p in range(phases):
        cols = slice(p * pc, (p + 1) * pc)
        if sent_taps:
            load(0, p).wait()
            for e in range(he):
                part = taps[e * LANES:(e + 1) * LANES, cols].astype(jnp.float32)
                stage_h[pl.ds(e, pc, stride=he), :] = part.T
            put(stage_h, hm, p, he)
        load(1, p).wait()
        load(2, p).wait()
        for a in range(blocks):
            span = slice(a * LANES, (a + 1) * LANES)
            part = gate[span, cols].astype(jnp.float32) * value[span, cols].astype(jnp.float32)
            stage_x[pl.ds(a, pc, stride=blocks), :] = part.T
        put(stage_x, xm, p, blocks)
        if p == 0:
            pl.semaphore_wait(barrier, n - 1 + m - 1)
        for g in range(p * per_phase, (p + 1) * per_phase):
            for kind in forward:
                for i in range(n - 1):
                    remote(kind, g, peer(kind, i)).start()
                own(kind, g).start()

    if not sent_taps:
        whole_taps.wait()
    og_load.wait()
    skip_load.wait()
    for a in range(blocks):
        span = slice(a * LANES, (a + 1) * LANES)
        ogt[pl.ds(a, channels, stride=blocks), :] = og[span, :].astype(jnp.float32).T
    xpad[:, :nd, :] = jnp.zeros((2, nd, LANES), jnp.float32)

    lane = lax.broadcasted_iota(jnp.int32, (16, LANES), 1)
    sub = lax.broadcasted_iota(jnp.int32, (16, LANES), 0)
    total = n * blocks

    def toeplitz(c):
        lines = []
        for d in range(nd):
            source = hf if sent_taps else taps
            line = source[d // he, pl.ds(c * he + d % he, 1), :]
            line = jnp.broadcast_to(line, (16, LANES))
            lines.append(pltpu.roll(line, 0, 1, stride=1, stride_axis=0))
        zero = jnp.zeros((16, LANES), jnp.float32)
        first = []
        for d in range(nd + 1):
            here = lines[d] if d < nd else zero
            before = lines[d - 1] if d > 0 else zero
            first.append(jnp.where(lane >= sub, here, before).astype(jnp.bfloat16))
        none = jnp.zeros((16, LANES), jnp.bfloat16)
        tiles = []
        turned = [[(f if q == 0 else pltpu.roll(f, 16 * q, 1)) for q in range(8)] for f in first]
        for d in range(nd + 1):
            rows = []
            for q in range(8):
                before = turned[d - 1][q] if d > 0 else none
                rows.append(turned[d][q] if q == 0 else jnp.where(lane >= 16 * q, turned[d][q], before))
            tiles.append(jnp.concatenate(rows, axis=0))
        return tiles

    def one_pair(g, p):
        c0 = g * width + 2 * p
        start = pl.multiple_of(c0 * blocks, 2 * blocks)
        both = xr[:, pl.ds(start, 2 * blocks), :].astype(jnp.float32)
        results = []
        for e in range(2):
            rows = both[:, e * blocks:(e + 1) * blocks, :].reshape(total, LANES)
            xpad[e, nd:, :] = rows
            tiles = toeplitz(c0 + e)
            acc = rows * skip[g * n * width + me * width + 2 * p + e]
            for d in range(0, nd + 1, 2):
                ds = [d, d + 1] if d + 1 <= nd else [d]
                left = [xpad[e, nd - x:nd - x + total, :].astype(jnp.bfloat16) for x in ds]
                left = left[0] if len(ds) == 1 else jnp.concatenate(left, axis=1)
                right = tiles[d] if len(ds) == 1 else jnp.concatenate([tiles[d], tiles[d + 1]], axis=0)
                acc = acc + jnp.dot(left, right, preferred_element_type=jnp.float32)
            results.append(acc.reshape(n, blocks, LANES))
        rs[:, pl.ds(start, 2 * blocks), :] = jnp.concatenate(results, axis=1).astype(jnp.bfloat16)

    for g in range(groups):
        for kind in forward:
            own(kind, g).wait()
            for i in range(n - 1):
                arrival(kind, g, peer(kind, i)).wait_recv()
        if sent_taps:
            rows = rows_of(TAPS, g)
            hf[:, rows, :] = hr[:, rows, :].astype(jnp.float32)

        def step(p, carry):
            one_pair(g, p)
            return carry

        lax.fori_loop(0, width // 2, step, 0)
        for i in range(n - 1):
            remote(RESULT, g, peer(RESULT, i)).start()
        own(RESULT, g).start()

    power[...] = jnp.zeros_like(power)
    span = width * blocks
    for g in range(groups):
        own(RESULT, g).wait()
        for i in range(n - 1):
            arrival(RESULT, g, peer(GATED, i)).wait_recv()

        def gather(d, carry):
            rows = rows_of(RESULT, g)
            at = pl.multiple_of((g * n + d) * span, span)
            piece = ogt[pl.ds(at, span), :] * cr[d, rows, :].astype(jnp.float32)
            mixed[pl.ds(at, span), :] = piece
            square = (piece * piece).reshape(width, blocks, LANES)
            power[...] += jnp.sum(square, axis=0)
            return carry

        lax.fori_loop(0, n, gather, 0)

    def exchange(k, incoming):
        other = lax.rem(mine + m - k, m) if incoming else mp_peer(mine, k, m)
        return pltpu.make_async_remote_copy(
            src_ref=power,
            dst_ref=powers.at[other if incoming else mine],
            send_sem=psend_sem.at[k],
            recv_sem=precv_sem.at[k],
            device_id={"mp": other},
            device_id_type=MESH,
        )

    for k in range(1, m):
        exchange(k, False).start()
    for kind in forward + [RESULT]:
        for g in range(groups):
            for i in range(n - 1):
                remote(kind, g, peer(kind, i)).wait_send()
    for k in range(1, m):
        exchange(k, True).wait_recv()
    add = power[...]
    for k in range(1, m):
        add = add + powers[lax.rem(mine + m - k, m)]
    sums[...] = add
    for k in range(1, m):
        exchange(k, False).wait_send()


def finish(blocks, channels, total_c, mixed, sums, out, held, out_sem):
    scale = 1.0 / jnp.sqrt(sums[...] / total_c + EPS)

    def store(a):
        span = slice(a * LANES, (a + 1) * LANES)
        return pltpu.make_async_copy(held.at[span], out.at[span], out_sem.at[a])

    for a in range(blocks):
        part = mixed[pl.ds(a, channels, stride=blocks), :] * scale[a:a + 1, :]
        held[a * LANES:(a + 1) * LANES, :] = part.T.astype(jnp.bfloat16)
        store(a).start()
    for a in range(blocks):
        store(a).wait()


def solution(mesh):
    n, m = mesh.shape["seq"], mesh.shape["mp"]

    def local(gate_in, value_in, out_gate, filter_taps, skip_gain):
        tokens, channels = gate_in.shape
        blocks = tokens // LANES
        cl = channels // n
        width = min(cl, 8)
        groups = cl // width
        phases = channels // max(LANES, n * width)
        own_taps = filter_taps.shape[0]
        sent_taps = own_taps % LANES == 0 and (width * (own_taps // LANES)) % 16 == 0
        nd = own_taps * n // LANES
        if sent_taps:
            hs, he, taps = n, own_taps // LANES, filter_taps
        else:
            hs, he = 1, nd
            dealt = filter_taps.reshape(own_taps, groups, n, width).swapaxes(1, 2).reshape(own_taps, channels)
            moved = lax.all_to_all(dealt, "seq", split_axis=1, concat_axis=0, tiled=True)
            taps = moved.astype(jnp.float32).T.reshape(1, cl * nd, LANES)
        cfg = (n, m, channels, blocks, cl, width, groups, phases, sent_taps, hs, he, channels * m)
        message = (n, cl * blocks, LANES)
        taps_message = (n, cl * he, LANES) if sent_taps else (n, 16, LANES)
        taps_stage = (channels // phases * he, LANES) if sent_taps else (16, LANES)
        mixed, sums = pl.pallas_call(
            functools.partial(kernel, cfg),
            out_shape=[
                pltpu.VMEM((channels * blocks, LANES), jnp.float32),
                pltpu.VMEM((blocks, LANES), jnp.float32),
            ],
            in_specs=[pl.BlockSpec(memory_space=pltpu.HBM)] * 5,
            out_specs=[pl.BlockSpec(memory_space=pltpu.VMEM)] * 2,
            scratch_shapes=[
                pltpu.VMEM(gate_in.shape, gate_in.dtype),
                pltpu.VMEM(value_in.shape, value_in.dtype),
                pltpu.VMEM(out_gate.shape, out_gate.dtype),
                pltpu.VMEM(taps.shape, taps.dtype),
                pltpu.SMEM(skip_gain.shape, skip_gain.dtype),
                pltpu.VMEM(taps_stage, jnp.float32),
                pltpu.VMEM((channels // phases * blocks, LANES), jnp.float32),
                pltpu.VMEM(message, jnp.bfloat16),
                pltpu.VMEM(taps_message, jnp.bfloat16),
                pltpu.VMEM(message, jnp.bfloat16),
                pltpu.VMEM(taps_message, jnp.bfloat16),
                pltpu.VMEM(taps_message, jnp.float32),
                pltpu.VMEM((2, nd + n * blocks, LANES), jnp.float32),
                pltpu.VMEM(message, jnp.bfloat16),
                pltpu.VMEM(message, jnp.bfloat16),
                pltpu.VMEM((channels * blocks, LANES), jnp.float32),
                pltpu.VMEM((blocks, LANES), jnp.float32),
                pltpu.VMEM((m, blocks, LANES), jnp.float32),
                pltpu.SemaphoreType.DMA((5, phases)),
                pltpu.SemaphoreType.DMA((3, groups, n)),
                pltpu.SemaphoreType.DMA((3, groups, n)),
                pltpu.SemaphoreType.DMA((3, groups)),
                pltpu.SemaphoreType.DMA((m,)),
                pltpu.SemaphoreType.DMA((m,)),
            ],
            compiler_params=pltpu.CompilerParams(
                collective_id=0, has_side_effects=True, vmem_limit_bytes=32 * 1024 * 1024
            ),
        )(*(pltpu.with_memory_space_constraint(x, pltpu.HBM) for x in (gate_in, value_in, out_gate, taps, skip_gain)))
        return pl.pallas_call(
            functools.partial(finish, blocks, channels, channels * m),
            out_shape=jax.ShapeDtypeStruct((tokens, channels), jnp.bfloat16),
            in_specs=[pl.BlockSpec(memory_space=pltpu.VMEM)] * 2,
            out_specs=pl.BlockSpec(memory_space=pltpu.HBM),
            scratch_shapes=[
                pltpu.VMEM((tokens, channels), jnp.bfloat16),
                pltpu.SemaphoreType.DMA((blocks,)),
            ],
            compiler_params=pltpu.CompilerParams(vmem_limit_bytes=8 * 1024 * 1024),
        )(mixed, sums)

    return jax.shard_map(
        local,
        mesh=mesh,
        in_specs=(P("seq", "mp"), P("seq", "mp"), P("seq", "mp"), P("seq", "mp"), P("mp")),
        out_specs=P("seq", "mp"),
        check_vma=False,
    )
```

```python
import functools

import jax
import jax.numpy as jnp
from jax import lax
from jax.experimental import pallas as pl
from jax.experimental.pallas import tpu as pltpu
from jax.sharding import PartitionSpec as P

MESH = pl.DeviceIdType.MESH
LANES = 128
FORWARD, RESULT = 0, 1
EPS = 1e-05
MESSAGE = 16
RETURN = 16


def forward_peer(me, i, n):
    if n & (n - 1) == 0:
        return me ^ (n - 1 - i)
    return lax.rem(me + 1 + i, n)


def result_peer(me, i, n):
    if n & (n - 1) or n < 4:
        return lax.rem(me + 1 + i, n)
    odd = lax.rem(me, 2)
    return jnp.where(i < me - odd, i, i + 1) ^ odd


def mp_peer(mine, k, m):
    return lax.rem(mine + k, m)


def tap_tiles(line_of, nd):
    lane = lax.broadcasted_iota(jnp.int32, (16, LANES), 1)
    sub = lax.broadcasted_iota(jnp.int32, (16, LANES), 0)
    zero = jnp.zeros((16, LANES), jnp.float32)
    none = zero.astype(jnp.bfloat16)
    lines = []
    for d in range(nd):
        line = jnp.broadcast_to(line_of(d), (16, LANES))
        lines.append(pltpu.roll(line, 0, 1, stride=1, stride_axis=0))
    first = []
    for d in range(nd + 1):
        here = lines[d] if d < nd else zero
        before = lines[d - 1] if d > 0 else zero
        first.append(jnp.where(lane >= sub, here, before).astype(jnp.bfloat16))
    bands = [first]
    for q in range(1, 4):
        turned = [pltpu.roll(f, 16 * q, 1) for f in first]
        bands.append([jnp.where(lane >= 16 * q, turned[d], turned[d - 1] if d else none) for d in range(nd + 1)])

    def tile(step):
        d = 2 * step
        return jnp.concatenate([
            jnp.concatenate([band[d] if d <= nd else none, band[d + 1] if d + 1 <= nd else none], axis=1)
            for band in bands
        ], axis=0)

    return [tile(step) for step in range(nd // 2 + 1)]


def convolve(x, tiles, even, odd, late):
    total = x.shape[0]
    pad = even.shape[0] - total
    lane = lax.broadcasted_iota(jnp.int32, (total, LANES), 1)
    turned = pltpu.roll(x, 64, 1)
    even[pad:, :] = x
    odd[pad:, :] = turned
    x_late = even[pad - 2:pad - 2 + total, :]
    turned_late = odd[pad - 2:pad - 2 + total, :]
    even[pad:, :] = jnp.where(lane < 64, x, turned_late)
    odd[pad:, :] = jnp.where(lane < 64, turned, x_late)
    left = []
    for step in range(0, tiles.shape[0] // 64, 2):
        at = pad - 2 * step
        left.append(jnp.concatenate([even[at:at + total, :], odd[at:at + total, :]], axis=0).astype(jnp.bfloat16))
    sums = jnp.dot(jnp.concatenate(left, axis=1), tiles[...], preferred_element_type=jnp.float32)
    late[0, 8:8 + total, :] = sums[:total, LANES:]
    late[1, 8:8 + total, :] = sums[total:, LANES:]
    even_late = late[0, 7:7 + total, :]
    odd_late = late[1, 7:7 + total, :]
    straddling = pltpu.roll(sums[total:, :LANES] + odd_late, 64, 1)
    late[1, 8:8 + total, :] = straddling
    return sums[:total, :LANES] + even_late + jnp.where(lane >= 64, straddling, late[1, 7:7 + total, :])


def kernel(cfg, gate_in, value_in, og_in, taps_in, skip_in, mixed, sums, gate, value, og, taps, skip, stage_h,
           stage_x, fm, fr, hf, tiles_a, tiles_b, even, odd, late, rs, cr, ogt, power, powers,
           load_sem, send_sem, recv_sem, own_sem, psend_sem, precv_sem):
    n, m, channels, blocks, cl, width, groups, phases, returns, sent_taps, hs, he, total_c = cfg
    me = lax.axis_index("seq")
    mine = lax.axis_index("mp")
    nd = hs * he
    pc = channels // phases
    sent = he if sent_taps else 0
    per = sent + blocks
    per_phase = groups // phases

    def load(i, p):
        src, dst = [(taps_in, taps), (gate_in, gate), (value_in, value)][i]
        cols = slice(p * pc, (p + 1) * pc)
        return pltpu.make_async_copy(src.at[:, cols], dst.at[:, cols], load_sem.at[i, p])

    og_load = pltpu.make_async_copy(og_in, og, load_sem.at[3, 0])
    skip_load = pltpu.make_async_copy(skip_in, skip, load_sem.at[4, 0])
    for p in range(phases):
        for i in ([0, 1, 2] if sent_taps else [1, 2]):
            load(i, p).start()
    if not sent_taps:
        whole_taps = pltpu.make_async_copy(taps_in, taps, load_sem.at[0, 0])
        whole_taps.start()

    barrier = pltpu.get_barrier_semaphore()
    for i in range(n - 1):
        pl.semaphore_signal(barrier, inc=1, device_id={"seq": forward_peer(me, i, n)}, device_id_type=MESH)
    for k in range(1, m):
        pl.semaphore_signal(barrier, inc=1, device_id={"mp": mp_peer(mine, k, m)}, device_id_type=MESH)
    og_load.start()
    skip_load.start()

    def rows_of(kind, g):
        if kind == RESULT:
            return pl.ds(g * returns * blocks, returns * blocks)
        return pl.ds(g * width * per, width * per)

    refs = {FORWARD: (fm, fr), RESULT: (rs, cr)}

    def remote(kind, g, to):
        src, dst = refs[kind]
        rows = rows_of(kind, g)
        return pltpu.make_async_remote_copy(
            src_ref=src.at[to, rows],
            dst_ref=dst.at[me, rows],
            send_sem=send_sem.at[kind, g, to],
            recv_sem=recv_sem.at[kind, g, me],
            device_id={"seq": to},
            device_id_type=MESH,
        )

    def arrival(kind, g, whence):
        src, dst = refs[kind]
        rows = rows_of(kind, g)
        return pltpu.make_async_remote_copy(
            src_ref=src.at[whence, rows],
            dst_ref=dst.at[whence, rows],
            send_sem=send_sem.at[kind, g, whence],
            recv_sem=recv_sem.at[kind, g, whence],
            device_id={"seq": whence},
            device_id_type=MESH,
        )

    def own(kind, g):
        src, dst = refs[kind]
        rows = rows_of(kind, g)
        return pltpu.make_async_copy(src.at[me, rows], dst.at[me, rows], own_sem.at[kind, g])

    everyone = [forward_peer(me, i, n) for i in range(n - 1)]
    in_turn = [result_peer(me, i, n) for i in range(n - 1)]

    def put(stage, p, offset, rows):
        for q in range(per_phase):
            g = p * per_phase + q
            size = n * width * rows
            part = stage[q * size:(q + 1) * size, :].astype(jnp.bfloat16)
            at = g * width * per + offset
            fm[:, at:at + width * rows, :] = part.reshape(n, width * rows, LANES)

    def send_forward(g):
        for to in everyone:
            remote(FORWARD, g, to).start()
        own(FORWARD, g).start()

    for p in range(phases):
        cols = slice(p * pc, (p + 1) * pc)
        if sent_taps:
            load(0, p).wait()
            for e in range(he):
                part = taps[e * LANES:(e + 1) * LANES, cols].astype(jnp.float32)
                stage_h[pl.ds(e, pc, stride=he), :] = part.T
            put(stage_h, p, 0, he)
        load(1, p).wait()
        load(2, p).wait()
        for a in range(blocks):
            span = slice(a * LANES, (a + 1) * LANES)
            part = gate[span, cols].astype(jnp.float32) * value[span, cols].astype(jnp.float32)
            stage_x[pl.ds(a, pc, stride=blocks), :] = part.T
        put(stage_x, p, width * sent, blocks)
        if p == 0:
            pl.semaphore_wait(barrier, n - 1 + m - 1)
        for g in range(p * per_phase, (p + 1) * per_phase):
            send_forward(g)

    if not sent_taps:
        whole_taps.wait()
    og_load.wait()
    skip_load.wait()
    for a in range(blocks):
        span = slice(a * LANES, (a + 1) * LANES)
        ogt[pl.ds(a, channels, stride=blocks), :] = og[span, :].astype(jnp.float32).T
    total = n * blocks
    pad = even.shape[1] - total
    even[:, :pad, :] = jnp.zeros((4, pad, LANES), jnp.float32)
    odd[:, :pad, :] = jnp.zeros((4, pad, LANES), jnp.float32)
    late[:, :, :8, :] = jnp.zeros((4, 2, 8, LANES), jnp.float32)
    reach = 64 * (nd // 2 + 1)
    for tiles in (tiles_a, tiles_b):
        if tiles.shape[1] > reach:
            tiles[:, reach:, :] = jnp.zeros((2, tiles.shape[1] - reach, 2 * LANES), jnp.bfloat16)

    filters = hf if sent_taps else taps

    def build(pair, tiles):
        for e in range(2):
            def line_of(d):
                return filters[d // he, pl.ds((2 * pair + e) * he + d % he, 1), :]

            for i, tile in enumerate(tap_tiles(line_of, nd)):
                tiles[e, 64 * i:64 * (i + 1), :] = tile

    def apply(g, p, tiles, half):
        pair = g * (width // 2) + p
        begin = pl.multiple_of(g * width * per + width * sent + 2 * blocks * p, 16)
        start = pl.multiple_of(2 * blocks * pair, 16)
        both = fr[:, pl.ds(begin, 2 * blocks), :].astype(jnp.float32)
        results = []
        for e in range(2):
            x = both[:, e * blocks:(e + 1) * blocks, :].reshape(total, LANES)
            at = 2 * half + e
            y = convolve(x, tiles.at[e], even.at[at], odd.at[at], late.at[at])
            y = y + x * skip[g * n * width + me * width + 2 * p + e]
            results.append(y.reshape(n, blocks, LANES))
        rs[:, pl.ds(start, 2 * blocks), :] = jnp.concatenate(results, axis=1).astype(jnp.bfloat16)

    last = width // 2 - 1
    per_group = width // returns
    for g in range(groups):
        own(FORWARD, g).wait()
        for whence in everyone:
            arrival(FORWARD, g, whence).wait_recv()
        if sent_taps:
            rows = pl.ds(g * width * per, width * sent)
            hf[:, g * width * he:(g + 1) * width * he, :] = fr[:, rows, :].astype(jnp.float32)
        first = g * (width // 2)
        build(first, tiles_a)

        def step(i, carry):
            apply(g, 2 * i, tiles_a, 0)
            build(first + 2 * i + 1, tiles_b)
            apply(g, 2 * i + 1, tiles_b, 1)
            build(first + jnp.minimum(2 * i + 2, last), tiles_a)
            return carry

        for r in range(per_group):
            lax.fori_loop(r * returns // 4, (r + 1) * returns // 4, step, 0)
            for to in in_turn:
                remote(RESULT, g * per_group + r, to).start()
            own(RESULT, g * per_group + r).start()

    power[...] = jnp.zeros_like(power)
    span = returns * blocks
    for g in range(groups * per_group):
        own(RESULT, g).wait()
        for whence in everyone:
            arrival(RESULT, g, whence).wait_recv()

        def gather(d, carry):
            at = ((g // per_group) * n + d) * width * blocks + (g % per_group) * span
            at = pl.multiple_of(at, span)
            piece = ogt[pl.ds(at, span), :] * cr[d, rows_of(RESULT, g), :].astype(jnp.float32)
            mixed[pl.ds(at, span), :] = piece
            square = (piece * piece).reshape(returns, blocks, LANES)
            power[...] += jnp.sum(square, axis=0)
            return carry

        lax.fori_loop(0, n, gather, 0)

    def exchange(k, incoming):
        other = lax.rem(mine + m - k, m) if incoming else mp_peer(mine, k, m)
        return pltpu.make_async_remote_copy(
            src_ref=power,
            dst_ref=powers.at[other if incoming else mine],
            send_sem=psend_sem.at[k],
            recv_sem=precv_sem.at[k],
            device_id={"mp": other},
            device_id_type=MESH,
        )

    for k in range(1, m):
        exchange(k, False).start()
    for g in range(groups):
        for to in everyone:
            remote(FORWARD, g, to).wait_send()
    for g in range(groups * per_group):
        for to in in_turn:
            remote(RESULT, g, to).wait_send()
    for k in range(1, m):
        exchange(k, True).wait_recv()
    add = power[...]
    for k in range(1, m):
        add = add + powers[lax.rem(mine + m - k, m)]
    sums[...] = add
    for k in range(1, m):
        exchange(k, False).wait_send()


def finish(blocks, channels, total_c, mixed, sums, out, held, out_sem):
    scale = 1.0 / jnp.sqrt(sums[...] / total_c + EPS)

    def store(a):
        span = slice(a * LANES, (a + 1) * LANES)
        return pltpu.make_async_copy(held.at[span], out.at[span], out_sem.at[a])

    for a in range(blocks):
        part = mixed[pl.ds(a, channels, stride=blocks), :] * scale[a:a + 1, :]
        held[a * LANES:(a + 1) * LANES, :] = part.T.astype(jnp.bfloat16)
        store(a).start()
    for a in range(blocks):
        store(a).wait()


def solution(mesh):
    n, m = mesh.shape["seq"], mesh.shape["mp"]

    def local(gate_in, value_in, out_gate, filter_taps, skip_gain):
        tokens, channels = gate_in.shape
        blocks = tokens // LANES
        cl = channels // n
        width = min(cl, MESSAGE)
        groups = cl // width
        phases = channels // max(LANES, n * width)
        own_taps = filter_taps.shape[0]
        sent_taps = own_taps % LANES == 0 and (width * (own_taps // LANES)) % 16 == 0
        nd = own_taps * n // LANES
        if sent_taps:
            hs, he, taps = n, own_taps // LANES, filter_taps
        else:
            hs, he = 1, nd
            dealt = filter_taps.reshape(own_taps, groups, n, width).swapaxes(1, 2).reshape(own_taps, channels)
            moved = lax.all_to_all(dealt, "seq", split_axis=1, concat_axis=0, tiled=True)
            taps = moved.astype(jnp.float32).T.reshape(1, cl * nd, LANES)
        returns = min(width, RETURN)
        pad = -(-(nd + 2) // 8) * 8
        depth = (nd // 2 + 2) // 2 * 128
        cfg = (n, m, channels, blocks, cl, width, groups, phases, returns, sent_taps, hs, he, channels * m)
        message = (n, cl * blocks, LANES)
        taps_message = (n, cl * he, LANES) if sent_taps else (1, 16, LANES)
        both_message = (n, cl * (blocks + (he if sent_taps else 0)), LANES)
        taps_stage = (channels // phases * he, LANES) if sent_taps else (16, LANES)
        mixed, sums = pl.pallas_call(
            functools.partial(kernel, cfg),
            out_shape=[
                pltpu.VMEM((channels * blocks, LANES), jnp.float32),
                pltpu.VMEM((blocks, LANES), jnp.float32),
            ],
            in_specs=[pl.BlockSpec(memory_space=pltpu.HBM)] * 5,
            out_specs=[pl.BlockSpec(memory_space=pltpu.VMEM)] * 2,
            scratch_shapes=[
                pltpu.VMEM(gate_in.shape, gate_in.dtype),
                pltpu.VMEM(value_in.shape, value_in.dtype),
                pltpu.VMEM(out_gate.shape, out_gate.dtype),
                pltpu.VMEM(taps.shape, taps.dtype),
                pltpu.SMEM(skip_gain.shape, skip_gain.dtype),
                pltpu.VMEM(taps_stage, jnp.float32),
                pltpu.VMEM((channels // phases * blocks, LANES), jnp.float32),
                pltpu.VMEM(both_message, jnp.bfloat16),
                pltpu.VMEM(both_message, jnp.bfloat16),
                pltpu.VMEM(taps_message, jnp.float32),
                pltpu.VMEM((2, depth, 2 * LANES), jnp.bfloat16),
                pltpu.VMEM((2, depth, 2 * LANES), jnp.bfloat16),
                pltpu.VMEM((4, pad + n * blocks, LANES), jnp.float32),
                pltpu.VMEM((4, pad + n * blocks, LANES), jnp.float32),
                pltpu.VMEM((4, 2, 8 + n * blocks, LANES), jnp.float32),
                pltpu.VMEM(message, jnp.bfloat16),
                pltpu.VMEM(message, jnp.bfloat16),
                pltpu.VMEM((channels * blocks, LANES), jnp.float32),
                pltpu.VMEM((blocks, LANES), jnp.float32),
                pltpu.VMEM((m, blocks, LANES), jnp.float32),
                pltpu.SemaphoreType.DMA((5, phases)),
                pltpu.SemaphoreType.DMA((2, cl // returns, n)),
                pltpu.SemaphoreType.DMA((2, cl // returns, n)),
                pltpu.SemaphoreType.DMA((2, cl // returns)),
                pltpu.SemaphoreType.DMA((m,)),
                pltpu.SemaphoreType.DMA((m,)),
            ],
            compiler_params=pltpu.CompilerParams(
                collective_id=0, has_side_effects=True, vmem_limit_bytes=32 * 1024 * 1024
            ),
        )(*(pltpu.with_memory_space_constraint(x, pltpu.HBM) for x in (gate_in, value_in, out_gate, taps, skip_gain)))
        return pl.pallas_call(
            functools.partial(finish, blocks, channels, channels * m),
            out_shape=jax.ShapeDtypeStruct((tokens, channels), jnp.bfloat16),
            in_specs=[pl.BlockSpec(memory_space=pltpu.VMEM)] * 2,
            out_specs=pl.BlockSpec(memory_space=pltpu.HBM),
            scratch_shapes=[
                pltpu.VMEM((tokens, channels), jnp.bfloat16),
                pltpu.SemaphoreType.DMA((blocks,)),
            ],
            compiler_params=pltpu.CompilerParams(vmem_limit_bytes=8 * 1024 * 1024),
        )(mixed, sums)

    return jax.shard_map(
        local,
        mesh=mesh,
        in_specs=(P("seq", "mp"), P("seq", "mp"), P("seq", "mp"), P("seq", "mp"), P("mp")),
        out_specs=P("seq", "mp"),
        check_vma=False,
    )
```

```python
import functools

import jax
import jax.numpy as jnp
from jax import lax
from jax.experimental import pallas as pl
from jax.experimental.pallas import tpu as pltpu
from jax.sharding import PartitionSpec as P

MESH = pl.DeviceIdType.MESH
LANES = 128
FORWARD, RESULT = 0, 1
EPS = 1e-05
MESSAGE = 16
RETURN = 16


def forward_peer(me, i, n):
    if n & (n - 1) == 0:
        return me ^ (n - 1 - i)
    return lax.rem(me + 1 + i, n)


def result_peer(me, i, n):
    if n & (n - 1) or n < 4:
        return lax.rem(me + 1 + i, n)
    odd = lax.rem(me, 2)
    return jnp.where(i < me - odd, i, i + 1) ^ odd


def mp_peer(mine, k, m):
    return lax.rem(mine + k, m)


def tap_tiles(line_of, nd):
    lane = lax.broadcasted_iota(jnp.int32, (16, LANES), 1)
    sub = lax.broadcasted_iota(jnp.int32, (16, LANES), 0)
    zero = jnp.zeros((16, LANES), jnp.float32)
    none = zero.astype(jnp.bfloat16)
    lines = []
    for d in range(nd):
        line = jnp.broadcast_to(line_of(d), (16, LANES))
        lines.append(pltpu.roll(line, 0, 1, stride=1, stride_axis=0))
    first = []
    for d in range(nd + 1):
        here = lines[d] if d < nd else zero
        before = lines[d - 1] if d > 0 else zero
        first.append(jnp.where(lane >= sub, here, before).astype(jnp.bfloat16))
    bands = [first]
    for q in range(1, 4):
        turned = [pltpu.roll(f, 16 * q, 1) for f in first]
        bands.append([jnp.where(lane >= 16 * q, turned[d], turned[d - 1] if d else none) for d in range(nd + 1)])

    def tile(step):
        d = 2 * step
        return jnp.concatenate([
            jnp.concatenate([band[d] if d <= nd else none, band[d + 1] if d + 1 <= nd else none], axis=1)
            for band in bands
        ], axis=0)

    return [tile(step) for step in range(nd // 2 + 1)]


def convolve(x, tiles, even, odd, late):
    total = x.shape[0]
    pad = even.shape[0] - total
    lane = lax.broadcasted_iota(jnp.int32, (total, LANES), 1)
    turned = pltpu.roll(x, 64, 1)
    even[pad:, :] = x
    odd[pad:, :] = turned
    x_late = even[pad - 2:pad - 2 + total, :]
    turned_late = odd[pad - 2:pad - 2 + total, :]
    even[pad:, :] = jnp.where(lane < 64, x, turned_late)
    odd[pad:, :] = jnp.where(lane < 64, turned, x_late)
    left = []
    for step in range(0, tiles.shape[0] // 64, 2):
        at = pad - 2 * step
        left.append(jnp.concatenate([even[at:at + total, :], odd[at:at + total, :]], axis=0).astype(jnp.bfloat16))
    sums = jnp.dot(jnp.concatenate(left, axis=1), tiles[...], preferred_element_type=jnp.float32)
    late[0, 8:8 + total, :] = sums[:total, LANES:]
    late[1, 8:8 + total, :] = sums[total:, LANES:]
    even_late = late[0, 7:7 + total, :]
    odd_late = late[1, 7:7 + total, :]
    straddling = pltpu.roll(sums[total:, :LANES] + odd_late, 64, 1)
    late[1, 8:8 + total, :] = straddling
    return sums[:total, :LANES] + even_late + jnp.where(lane >= 64, straddling, late[1, 7:7 + total, :])


def kernel(cfg, gate_in, value_in, og_in, taps_in, skip_in, turned, sums, gate, value, og, taps, skip, stage_h,
           stage_x, fm, fr, hf, tiles_a, tiles_b, even, odd, late, rs, cr, ogt, power, powers,
           load_sem, send_sem, recv_sem, own_sem, psend_sem, precv_sem, mixed):
    n, m, channels, blocks, cl, width, groups, phases, returns, sent_taps, hs, he, total_c = cfg
    me = lax.axis_index("seq")
    mine = lax.axis_index("mp")
    nd = hs * he
    pc = channels // phases
    sent = he if sent_taps else 0
    per = sent + blocks
    per_phase = groups // phases

    def load(i, p):
        src, dst = [(taps_in, taps), (gate_in, gate), (value_in, value)][i]
        cols = slice(p * pc, (p + 1) * pc)
        return pltpu.make_async_copy(src.at[:, cols], dst.at[:, cols], load_sem.at[i, p])

    og_load = pltpu.make_async_copy(og_in, og, load_sem.at[3, 0])
    skip_load = pltpu.make_async_copy(skip_in, skip, load_sem.at[4, 0])
    for p in range(phases):
        for i in ([0, 1, 2] if sent_taps else [1, 2]):
            load(i, p).start()
    if not sent_taps:
        whole_taps = pltpu.make_async_copy(taps_in, taps, load_sem.at[0, 0])
        whole_taps.start()

    barrier = pltpu.get_barrier_semaphore()
    for i in range(n - 1):
        pl.semaphore_signal(barrier, inc=1, device_id={"seq": forward_peer(me, i, n)}, device_id_type=MESH)
    for k in range(1, m):
        pl.semaphore_signal(barrier, inc=1, device_id={"mp": mp_peer(mine, k, m)}, device_id_type=MESH)
    og_load.start()
    skip_load.start()

    def rows_of(kind, g):
        if kind == RESULT:
            return pl.ds(g * returns * blocks, returns * blocks)
        return pl.ds(g * width * per, width * per)

    refs = {FORWARD: (fm, fr), RESULT: (rs, cr)}

    def remote(kind, g, to):
        src, dst = refs[kind]
        rows = rows_of(kind, g)
        return pltpu.make_async_remote_copy(
            src_ref=src.at[to, rows],
            dst_ref=dst.at[me, rows],
            send_sem=send_sem.at[kind, g, to],
            recv_sem=recv_sem.at[kind, g, me],
            device_id={"seq": to},
            device_id_type=MESH,
        )

    def arrival(kind, g, whence):
        src, dst = refs[kind]
        rows = rows_of(kind, g)
        return pltpu.make_async_remote_copy(
            src_ref=src.at[whence, rows],
            dst_ref=dst.at[whence, rows],
            send_sem=send_sem.at[kind, g, whence],
            recv_sem=recv_sem.at[kind, g, whence],
            device_id={"seq": whence},
            device_id_type=MESH,
        )

    def own(kind, g):
        src, dst = refs[kind]
        rows = rows_of(kind, g)
        return pltpu.make_async_copy(src.at[me, rows], dst.at[me, rows], own_sem.at[kind, g])

    everyone = [forward_peer(me, i, n) for i in range(n - 1)]
    in_turn = [result_peer(me, i, n) for i in range(n - 1)]

    def put(stage, p, offset, rows):
        for q in range(per_phase):
            g = p * per_phase + q
            size = n * width * rows
            part = stage[q * size:(q + 1) * size, :].astype(jnp.bfloat16)
            at = g * width * per + offset
            fm[:, at:at + width * rows, :] = part.reshape(n, width * rows, LANES)

    def send_forward(g):
        for to in everyone:
            remote(FORWARD, g, to).start()
        own(FORWARD, g).start()

    outer = lax.rem(mine, 2) == 0

    for p in range(phases):
        cols = slice(p * pc, (p + 1) * pc)
        if sent_taps:
            load(0, p).wait()
            for e in range(he):
                part = taps[e * LANES:(e + 1) * LANES, cols].astype(jnp.float32)
                stage_h[pl.ds(e, pc, stride=he), :] = part.T
            put(stage_h, p, 0, he)
        load(1, p).wait()
        load(2, p).wait()
        for a in range(blocks):
            span = slice(a * LANES, (a + 1) * LANES)
            part = gate[span, cols].astype(jnp.float32) * value[span, cols].astype(jnp.float32)
            stage_x[pl.ds(a, pc, stride=blocks), :] = part.T
        put(stage_x, p, width * sent, blocks)
        if p == 0:
            pl.semaphore_wait(barrier, n - 1 + m - 1)
        for g in range(p * per_phase, (p + 1) * per_phase):
            if g == 0:
                send_forward(g)
            else:
                pl.when(outer)(functools.partial(send_forward, g))

    if not sent_taps:
        whole_taps.wait()
    og_load.wait()
    skip_load.wait()
    for a in range(blocks):
        span = slice(a * LANES, (a + 1) * LANES)
        ogt[pl.ds(a, channels, stride=blocks), :] = og[span, :].astype(jnp.float32).T
    total = n * blocks
    pad = even.shape[1] - total
    even[:, :pad, :] = jnp.zeros((4, pad, LANES), jnp.float32)
    odd[:, :pad, :] = jnp.zeros((4, pad, LANES), jnp.float32)
    late[:, :, :8, :] = jnp.zeros((4, 2, 8, LANES), jnp.float32)
    reach = 64 * (nd // 2 + 1)
    for tiles in (tiles_a, tiles_b):
        if tiles.shape[1] > reach:
            tiles[:, reach:, :] = jnp.zeros((2, tiles.shape[1] - reach, 2 * LANES), jnp.bfloat16)

    filters = hf if sent_taps else taps

    def build(pair, tiles):
        for e in range(2):
            def line_of(d):
                return filters[d // he, pl.ds((2 * pair + e) * he + d % he, 1), :]

            for i, tile in enumerate(tap_tiles(line_of, nd)):
                tiles[e, 64 * i:64 * (i + 1), :] = tile

    def apply(g, p, tiles, half):
        pair = g * (width // 2) + p
        begin = pl.multiple_of(g * width * per + width * sent + 2 * blocks * p, 16)
        start = pl.multiple_of(2 * blocks * pair, 16)
        both = fr[:, pl.ds(begin, 2 * blocks), :].astype(jnp.float32)
        results = []
        for e in range(2):
            x = both[:, e * blocks:(e + 1) * blocks, :].reshape(total, LANES)
            at = 2 * half + e
            y = convolve(x, tiles.at[e], even.at[at], odd.at[at], late.at[at])
            y = y + x * skip[g * n * width + me * width + 2 * p + e]
            results.append(y.reshape(n, blocks, LANES))
        rs[:, pl.ds(start, 2 * blocks), :] = jnp.concatenate(results, axis=1).astype(jnp.bfloat16)

    last = width // 2 - 1
    per_group = width // returns
    for g in range(groups):
        own(FORWARD, g).wait()
        for whence in everyone:
            arrival(FORWARD, g, whence).wait_recv()
        if g + 1 < groups:
            pl.when(jnp.logical_not(outer))(functools.partial(send_forward, g + 1))
        if sent_taps:
            rows = pl.ds(g * width * per, width * sent)
            hf[:, g * width * he:(g + 1) * width * he, :] = fr[:, rows, :].astype(jnp.float32)
        first = g * (width // 2)
        build(first, tiles_a)

        def step(i, carry):
            apply(g, 2 * i, tiles_a, 0)
            build(first + 2 * i + 1, tiles_b)
            apply(g, 2 * i + 1, tiles_b, 1)
            build(first + jnp.minimum(2 * i + 2, last), tiles_a)
            return carry

        for r in range(per_group):
            lax.fori_loop(r * returns // 4, (r + 1) * returns // 4, step, 0)
            for to in in_turn:
                remote(RESULT, g * per_group + r, to).start()
            own(RESULT, g * per_group + r).start()

    power[...] = jnp.zeros_like(power)
    span = returns * blocks
    for g in range(groups * per_group):
        def gather(d):
            at = ((g // per_group) * n + d) * width * blocks + (g % per_group) * span
            at = pl.multiple_of(at, span)
            piece = ogt[pl.ds(at, span), :] * cr[d, rows_of(RESULT, g), :].astype(jnp.float32)
            mixed[pl.ds(at, span), :] = piece
            square = (piece * piece).reshape(returns, blocks, LANES)
            power[...] += jnp.sum(square, axis=0)

        own(RESULT, g).wait()
        gather(me)
        for whence in reversed(everyone):
            arrival(RESULT, g, whence).wait_recv()
            gather(whence)

    def exchange(k, incoming):
        other = lax.rem(mine + m - k, m) if incoming else mp_peer(mine, k, m)
        return pltpu.make_async_remote_copy(
            src_ref=power,
            dst_ref=powers.at[other if incoming else mine],
            send_sem=psend_sem.at[k],
            recv_sem=precv_sem.at[k],
            device_id={"mp": other},
            device_id_type=MESH,
        )

    for k in range(1, m):
        exchange(k, False).start()
    for a in range(blocks):
        turned[a * LANES:(a + 1) * LANES, :] = mixed[pl.ds(a, channels, stride=blocks), :].T
    for g in range(groups):
        for to in everyone:
            remote(FORWARD, g, to).wait_send()
    for g in range(groups * per_group):
        for to in in_turn:
            remote(RESULT, g, to).wait_send()
    for k in range(1, m):
        exchange(k, True).wait_recv()
    add = power[...]
    for k in range(1, m):
        add = add + powers[lax.rem(mine + m - k, m)]
    sums[...] = add
    for k in range(1, m):
        exchange(k, False).wait_send()


def finish(blocks, channels, total_c, turned, sums, out, held, out_sem):
    scale = 1.0 / jnp.sqrt(sums[...] / total_c + EPS)

    def store(a):
        span = slice(a * LANES, (a + 1) * LANES)
        return pltpu.make_async_copy(held.at[span], out.at[span], out_sem.at[a])

    for a in range(blocks):
        span = slice(a * LANES, (a + 1) * LANES)
        column = jnp.broadcast_to(scale[a:a + 1, :], (LANES, LANES)).T
        held[span, :] = (turned[span, :] * jnp.concatenate([column] * (channels // LANES), axis=1)).astype(jnp.bfloat16)
        store(a).start()
    for a in range(blocks):
        store(a).wait()


def solution(mesh):
    n, m = mesh.shape["seq"], mesh.shape["mp"]

    def local(gate_in, value_in, out_gate, filter_taps, skip_gain):
        tokens, channels = gate_in.shape
        blocks = tokens // LANES
        cl = channels // n
        width = min(cl, MESSAGE)
        groups = cl // width
        phases = channels // max(LANES, n * width)
        own_taps = filter_taps.shape[0]
        sent_taps = own_taps % LANES == 0 and (width * (own_taps // LANES)) % 16 == 0
        nd = own_taps * n // LANES
        if sent_taps:
            hs, he, taps = n, own_taps // LANES, filter_taps
        else:
            hs, he = 1, nd
            dealt = filter_taps.reshape(own_taps, groups, n, width).swapaxes(1, 2).reshape(own_taps, channels)
            moved = lax.all_to_all(dealt, "seq", split_axis=1, concat_axis=0, tiled=True)
            taps = moved.astype(jnp.float32).T.reshape(1, cl * nd, LANES)
        returns = min(width, RETURN)
        pad = -(-(nd + 2) // 8) * 8
        depth = (nd // 2 + 2) // 2 * 128
        cfg = (n, m, channels, blocks, cl, width, groups, phases, returns, sent_taps, hs, he, channels * m)
        message = (n, cl * blocks, LANES)
        taps_message = (n, cl * he, LANES) if sent_taps else (1, 16, LANES)
        both_message = (n, cl * (blocks + (he if sent_taps else 0)), LANES)
        taps_stage = (channels // phases * he, LANES) if sent_taps else (16, LANES)
        mixed, sums = pl.pallas_call(
            functools.partial(kernel, cfg),
            out_shape=[
                pltpu.VMEM((tokens, channels), jnp.float32),
                pltpu.VMEM((blocks, LANES), jnp.float32),
            ],
            in_specs=[pl.BlockSpec(memory_space=pltpu.HBM)] * 5,
            out_specs=[pl.BlockSpec(memory_space=pltpu.VMEM)] * 2,
            scratch_shapes=[
                pltpu.VMEM(gate_in.shape, gate_in.dtype),
                pltpu.VMEM(value_in.shape, value_in.dtype),
                pltpu.VMEM(out_gate.shape, out_gate.dtype),
                pltpu.VMEM(taps.shape, taps.dtype),
                pltpu.SMEM(skip_gain.shape, skip_gain.dtype),
                pltpu.VMEM(taps_stage, jnp.float32),
                pltpu.VMEM((channels // phases * blocks, LANES), jnp.float32),
                pltpu.VMEM(both_message, jnp.bfloat16),
                pltpu.VMEM(both_message, jnp.bfloat16),
                pltpu.VMEM(taps_message, jnp.float32),
                pltpu.VMEM((2, depth, 2 * LANES), jnp.bfloat16),
                pltpu.VMEM((2, depth, 2 * LANES), jnp.bfloat16),
                pltpu.VMEM((4, pad + n * blocks, LANES), jnp.float32),
                pltpu.VMEM((4, pad + n * blocks, LANES), jnp.float32),
                pltpu.VMEM((4, 2, 8 + n * blocks, LANES), jnp.float32),
                pltpu.VMEM(message, jnp.bfloat16),
                pltpu.VMEM(message, jnp.bfloat16),
                pltpu.VMEM((channels * blocks, LANES), jnp.float32),
                pltpu.VMEM((blocks, LANES), jnp.float32),
                pltpu.VMEM((m, blocks, LANES), jnp.float32),
                pltpu.SemaphoreType.DMA((5, phases)),
                pltpu.SemaphoreType.DMA((2, cl // returns, n)),
                pltpu.SemaphoreType.DMA((2, cl // returns, n)),
                pltpu.SemaphoreType.DMA((2, cl // returns)),
                pltpu.SemaphoreType.DMA((m,)),
                pltpu.SemaphoreType.DMA((m,)),
                pltpu.VMEM((channels * blocks, LANES), jnp.float32),
            ],
            compiler_params=pltpu.CompilerParams(
                collective_id=0, has_side_effects=True, vmem_limit_bytes=32 * 1024 * 1024
            ),
        )(*(pltpu.with_memory_space_constraint(x, pltpu.HBM) for x in (gate_in, value_in, out_gate, taps, skip_gain)))
        return pl.pallas_call(
            functools.partial(finish, blocks, channels, channels * m),
            out_shape=jax.ShapeDtypeStruct((tokens, channels), jnp.bfloat16),
            in_specs=[pl.BlockSpec(memory_space=pltpu.VMEM)] * 2,
            out_specs=pl.BlockSpec(memory_space=pltpu.HBM),
            scratch_shapes=[
                pltpu.VMEM((tokens, channels), jnp.bfloat16),
                pltpu.SemaphoreType.DMA((blocks,)),
            ],
            compiler_params=pltpu.CompilerParams(vmem_limit_bytes=8 * 1024 * 1024),
        )(mixed, sums)

    return jax.shard_map(
        local,
        mesh=mesh,
        in_specs=(P("seq", "mp"), P("seq", "mp"), P("seq", "mp"), P("seq", "mp"), P("mp")),
        out_specs=P("seq", "mp"),
        check_vma=False,
    )
```

```python
import functools

import jax
import jax.numpy as jnp
from jax import lax
from jax.experimental import pallas as pl
from jax.experimental.pallas import tpu as pltpu
from jax.sharding import PartitionSpec as P

MESH = pl.DeviceIdType.MESH
LANES = 128
FORWARD, RESULT = 0, 1
EPS = 1e-05
MESSAGE = 16
RETURN = 16


def forward_peer(me, i, n):
    if n & (n - 1) == 0:
        return me ^ (n - 1 - i)
    return lax.rem(me + 1 + i, n)


def result_peer(me, i, n):
    if n & (n - 1) or n < 4:
        return lax.rem(me + 1 + i, n)
    odd = lax.rem(me, 2)
    return jnp.where(i < me - odd, i, i + 1) ^ odd


def mp_peer(mine, k, m):
    return lax.rem(mine + k, m)


def tap_tiles(line_of, nd):
    lane = lax.broadcasted_iota(jnp.int32, (16, LANES), 1)
    sub = lax.broadcasted_iota(jnp.int32, (16, LANES), 0)
    zero = jnp.zeros((16, LANES), jnp.float32)
    none = zero.astype(jnp.bfloat16)
    lines = []
    for d in range(nd):
        line = jnp.broadcast_to(line_of(d), (16, LANES))
        lines.append(pltpu.roll(line, 0, 1, stride=1, stride_axis=0))
    first = []
    for d in range(nd + 1):
        here = lines[d] if d < nd else zero
        before = lines[d - 1] if d > 0 else zero
        first.append(jnp.where(lane >= sub, here, before).astype(jnp.bfloat16))
    bands = [first]
    for q in range(1, 4):
        turned = [pltpu.roll(f, 16 * q, 1) for f in first]
        bands.append([jnp.where(lane >= 16 * q, turned[d], turned[d - 1] if d else none) for d in range(nd + 1)])

    def tile(step):
        d = 2 * step
        return jnp.concatenate([
            jnp.concatenate([band[d] if d <= nd else none, band[d + 1] if d + 1 <= nd else none], axis=1)
            for band in bands
        ], axis=0)

    return [tile(step) for step in range(nd // 2 + 1)]


def convolve(x, tiles, even, odd, late):
    total = x.shape[0]
    pad = even.shape[0] - total
    lane = lax.broadcasted_iota(jnp.int32, (total, LANES), 1)
    turned = pltpu.roll(x, 64, 1)
    even[pad:, :] = x
    odd[pad:, :] = turned
    x_late = even[pad - 2:pad - 2 + total, :]
    turned_late = odd[pad - 2:pad - 2 + total, :]
    even[pad:, :] = jnp.where(lane < 64, x, turned_late)
    odd[pad:, :] = jnp.where(lane < 64, turned, x_late)
    left = []
    for step in range(0, tiles.shape[0] // 64, 2):
        at = pad - 2 * step
        left.append(jnp.concatenate([even[at:at + total, :], odd[at:at + total, :]], axis=0).astype(jnp.bfloat16))
    sums = jnp.dot(jnp.concatenate(left, axis=1), tiles[...], preferred_element_type=jnp.float32)
    late[0, 8:8 + total, :] = sums[:total, LANES:]
    late[1, 8:8 + total, :] = sums[total:, LANES:]
    even_late = late[0, 7:7 + total, :]
    odd_late = late[1, 7:7 + total, :]
    straddling = pltpu.roll(sums[total:, :LANES] + odd_late, 64, 1)
    late[1, 8:8 + total, :] = straddling
    return sums[:total, :LANES] + even_late + jnp.where(lane >= 64, straddling, late[1, 7:7 + total, :])


def kernel(cfg, gate_in, value_in, og_in, taps_in, skip_in, turned, sums, gate, value, og, taps, skip, stage_h,
           stage_x, fm, fr, hf, tiles_a, tiles_b, even, odd, late, rs, cr, ogt, power, powers,
           load_sem, send_sem, recv_sem, own_sem, psend_sem, precv_sem, mixed):
    n, m, channels, blocks, cl, width, groups, phases, returns, sent_taps, hs, he, total_c = cfg
    me = lax.axis_index("seq")
    mine = lax.axis_index("mp")
    nd = hs * he
    pc = channels // phases
    sent = he if sent_taps else 0
    per = sent + blocks
    per_phase = groups // phases

    def load(i, p):
        src, dst = [(taps_in, taps), (gate_in, gate), (value_in, value)][i]
        cols = slice(p * pc, (p + 1) * pc)
        return pltpu.make_async_copy(src.at[:, cols], dst.at[:, cols], load_sem.at[i, p])

    og_load = pltpu.make_async_copy(og_in, og, load_sem.at[3, 0])
    skip_load = pltpu.make_async_copy(skip_in, skip, load_sem.at[4, 0])
    for p in range(phases):
        for i in ([0, 1, 2] if sent_taps else [1, 2]):
            load(i, p).start()
    if not sent_taps:
        whole_taps = pltpu.make_async_copy(taps_in, taps, load_sem.at[0, 0])
        whole_taps.start()

    barrier = pltpu.get_barrier_semaphore()
    for i in range(n - 1):
        pl.semaphore_signal(barrier, inc=1, device_id={"seq": forward_peer(me, i, n)}, device_id_type=MESH)
    for k in range(1, m):
        pl.semaphore_signal(barrier, inc=1, device_id={"mp": mp_peer(mine, k, m)}, device_id_type=MESH)
    og_load.start()
    skip_load.start()

    def rows_of(kind, g):
        if kind == RESULT:
            return pl.ds(g * returns * blocks, returns * blocks)
        return pl.ds(g * width * per, width * per)

    refs = {FORWARD: (fm, fr), RESULT: (rs, cr)}

    def remote(kind, g, to):
        src, dst = refs[kind]
        rows = rows_of(kind, g)
        return pltpu.make_async_remote_copy(
            src_ref=src.at[to, rows],
            dst_ref=dst.at[me, rows],
            send_sem=send_sem.at[kind, g, to],
            recv_sem=recv_sem.at[kind, g, me],
            device_id={"seq": to},
            device_id_type=MESH,
        )

    def arrival(kind, g, whence):
        src, dst = refs[kind]
        rows = rows_of(kind, g)
        return pltpu.make_async_remote_copy(
            src_ref=src.at[whence, rows],
            dst_ref=dst.at[whence, rows],
            send_sem=send_sem.at[kind, g, whence],
            recv_sem=recv_sem.at[kind, g, whence],
            device_id={"seq": whence},
            device_id_type=MESH,
        )

    def own(kind, g):
        src, dst = refs[kind]
        rows = rows_of(kind, g)
        return pltpu.make_async_copy(src.at[me, rows], dst.at[me, rows], own_sem.at[kind, g])

    everyone = [forward_peer(me, i, n) for i in range(n - 1)]
    in_turn = [result_peer(me, i, n) for i in range(n - 1)]

    def put(stage, p, offset, rows):
        for q in range(per_phase):
            g = p * per_phase + q
            size = n * width * rows
            part = stage[q * size:(q + 1) * size, :].astype(jnp.bfloat16)
            at = g * width * per + offset
            fm[:, at:at + width * rows, :] = part.reshape(n, width * rows, LANES)

    def send_forward(g):
        for to in everyone:
            remote(FORWARD, g, to).start()
        own(FORWARD, g).start()

    outer = (lax.rem(mine, 2) == 0) & ((me < n // 4) | (me >= n - n // 4))

    for p in range(phases):
        cols = slice(p * pc, (p + 1) * pc)
        if sent_taps:
            load(0, p).wait()
            for e in range(he):
                part = taps[e * LANES:(e + 1) * LANES, cols].astype(jnp.float32)
                stage_h[pl.ds(e, pc, stride=he), :] = part.T
            put(stage_h, p, 0, he)
        load(1, p).wait()
        load(2, p).wait()
        for a in range(blocks):
            span = slice(a * LANES, (a + 1) * LANES)
            part = gate[span, cols].astype(jnp.float32) * value[span, cols].astype(jnp.float32)
            stage_x[pl.ds(a, pc, stride=blocks), :] = part.T
        put(stage_x, p, width * sent, blocks)
        if p == 0:
            pl.semaphore_wait(barrier, n - 1 + m - 1)
        for g in range(p * per_phase, (p + 1) * per_phase):
            if g == 0:
                send_forward(g)
            else:
                pl.when(outer)(functools.partial(send_forward, g))

    if not sent_taps:
        whole_taps.wait()
    og_load.wait()
    skip_load.wait()
    for a in range(blocks):
        span = slice(a * LANES, (a + 1) * LANES)
        ogt[pl.ds(a, channels, stride=blocks), :] = og[span, :].astype(jnp.float32).T
    total = n * blocks
    pad = even.shape[1] - total
    even[:, :pad, :] = jnp.zeros((4, pad, LANES), jnp.float32)
    odd[:, :pad, :] = jnp.zeros((4, pad, LANES), jnp.float32)
    late[:, :, :8, :] = jnp.zeros((4, 2, 8, LANES), jnp.float32)
    reach = 64 * (nd // 2 + 1)
    for tiles in (tiles_a, tiles_b):
        if tiles.shape[1] > reach:
            tiles[:, reach:, :] = jnp.zeros((2, tiles.shape[1] - reach, 2 * LANES), jnp.bfloat16)

    filters = hf if sent_taps else taps

    def build(pair, tiles):
        for e in range(2):
            def line_of(d):
                return filters[d // he, pl.ds((2 * pair + e) * he + d % he, 1), :]

            for i, tile in enumerate(tap_tiles(line_of, nd)):
                tiles[e, 64 * i:64 * (i + 1), :] = tile

    def apply(g, p, tiles, half):
        pair = g * (width // 2) + p
        begin = pl.multiple_of(g * width * per + width * sent + 2 * blocks * p, 16)
        start = pl.multiple_of(2 * blocks * pair, 16)
        both = fr[:, pl.ds(begin, 2 * blocks), :].astype(jnp.float32)
        results = []
        for e in range(2):
            x = both[:, e * blocks:(e + 1) * blocks, :].reshape(total, LANES)
            at = 2 * half + e
            y = convolve(x, tiles.at[e], even.at[at], odd.at[at], late.at[at])
            y = y + x * skip[g * n * width + me * width + 2 * p + e]
            results.append(y.reshape(n, blocks, LANES))
        rs[:, pl.ds(start, 2 * blocks), :] = jnp.concatenate(results, axis=1).astype(jnp.bfloat16)

    last = width // 2 - 1
    per_group = width // returns
    for g in range(groups):
        own(FORWARD, g).wait()
        for whence in everyone:
            arrival(FORWARD, g, whence).wait_recv()
        if g + 1 < groups:
            pl.when(jnp.logical_not(outer))(functools.partial(send_forward, g + 1))
        if sent_taps:
            rows = pl.ds(g * width * per, width * sent)
            hf[:, g * width * he:(g + 1) * width * he, :] = fr[:, rows, :].astype(jnp.float32)
        first = g * (width // 2)
        build(first, tiles_a)

        def step(i, carry):
            apply(g, 2 * i, tiles_a, 0)
            build(first + 2 * i + 1, tiles_b)
            apply(g, 2 * i + 1, tiles_b, 1)
            build(first + jnp.minimum(2 * i + 2, last), tiles_a)
            return carry

        for r in range(per_group):
            lax.fori_loop(r * returns // 4, (r + 1) * returns // 4, step, 0)
            for to in in_turn:
                remote(RESULT, g * per_group + r, to).start()
            own(RESULT, g * per_group + r).start()

    power[...] = jnp.zeros_like(power)
    span = returns * blocks
    for g in range(groups * per_group):
        def gather(d):
            at = ((g // per_group) * n + d) * width * blocks + (g % per_group) * span
            at = pl.multiple_of(at, span)
            piece = ogt[pl.ds(at, span), :] * cr[d, rows_of(RESULT, g), :].astype(jnp.float32)
            mixed[pl.ds(at, span), :] = piece
            square = (piece * piece).reshape(returns, blocks, LANES)
            power[...] += jnp.sum(square, axis=0)

        own(RESULT, g).wait()
        gather(me)
        for whence in reversed(everyone):
            arrival(RESULT, g, whence).wait_recv()
            gather(whence)

    def exchange(k, incoming):
        other = lax.rem(mine + m - k, m) if incoming else mp_peer(mine, k, m)
        return pltpu.make_async_remote_copy(
            src_ref=power,
            dst_ref=powers.at[other if incoming else mine],
            send_sem=psend_sem.at[k],
            recv_sem=precv_sem.at[k],
            device_id={"mp": other},
            device_id_type=MESH,
        )

    for k in range(1, m):
        exchange(k, False).start()
    for a in range(blocks):
        turned[a * LANES:(a + 1) * LANES, :] = mixed[pl.ds(a, channels, stride=blocks), :].T
    for g in range(groups):
        for to in everyone:
            remote(FORWARD, g, to).wait_send()
    for g in range(groups * per_group):
        for to in in_turn:
            remote(RESULT, g, to).wait_send()
    for k in range(1, m):
        exchange(k, True).wait_recv()
    add = power[...]
    for k in range(1, m):
        add = add + powers[lax.rem(mine + m - k, m)]
    sums[...] = add
    for k in range(1, m):
        exchange(k, False).wait_send()


def finish(blocks, channels, total_c, turned, sums, out, held, out_sem):
    scale = 1.0 / jnp.sqrt(sums[...] / total_c + EPS)

    def store(a):
        span = slice(a * LANES, (a + 1) * LANES)
        return pltpu.make_async_copy(held.at[span], out.at[span], out_sem.at[a])

    for a in range(blocks):
        span = slice(a * LANES, (a + 1) * LANES)
        column = jnp.broadcast_to(scale[a:a + 1, :], (LANES, LANES)).T
        held[span, :] = (turned[span, :] * jnp.concatenate([column] * (channels // LANES), axis=1)).astype(jnp.bfloat16)
        store(a).start()
    for a in range(blocks):
        store(a).wait()


def solution(mesh):
    n, m = mesh.shape["seq"], mesh.shape["mp"]

    def local(gate_in, value_in, out_gate, filter_taps, skip_gain):
        tokens, channels = gate_in.shape
        blocks = tokens // LANES
        cl = channels // n
        width = min(cl, MESSAGE)
        groups = cl // width
        phases = channels // max(LANES, n * width)
        own_taps = filter_taps.shape[0]
        sent_taps = own_taps % LANES == 0 and (width * (own_taps // LANES)) % 16 == 0
        nd = own_taps * n // LANES
        if sent_taps:
            hs, he, taps = n, own_taps // LANES, filter_taps
        else:
            hs, he = 1, nd
            dealt = filter_taps.reshape(own_taps, groups, n, width).swapaxes(1, 2).reshape(own_taps, channels)
            moved = lax.all_to_all(dealt, "seq", split_axis=1, concat_axis=0, tiled=True)
            taps = moved.astype(jnp.float32).T.reshape(1, cl * nd, LANES)
        returns = min(width, RETURN)
        pad = -(-(nd + 2) // 8) * 8
        depth = (nd // 2 + 2) // 2 * 128
        cfg = (n, m, channels, blocks, cl, width, groups, phases, returns, sent_taps, hs, he, channels * m)
        message = (n, cl * blocks, LANES)
        taps_message = (n, cl * he, LANES) if sent_taps else (1, 16, LANES)
        both_message = (n, cl * (blocks + (he if sent_taps else 0)), LANES)
        taps_stage = (channels // phases * he, LANES) if sent_taps else (16, LANES)
        mixed, sums = pl.pallas_call(
            functools.partial(kernel, cfg),
            out_shape=[
                pltpu.VMEM((tokens, channels), jnp.float32),
                pltpu.VMEM((blocks, LANES), jnp.float32),
            ],
            in_specs=[pl.BlockSpec(memory_space=pltpu.HBM)] * 5,
            out_specs=[pl.BlockSpec(memory_space=pltpu.VMEM)] * 2,
            scratch_shapes=[
                pltpu.VMEM(gate_in.shape, gate_in.dtype),
                pltpu.VMEM(value_in.shape, value_in.dtype),
                pltpu.VMEM(out_gate.shape, out_gate.dtype),
                pltpu.VMEM(taps.shape, taps.dtype),
                pltpu.SMEM(skip_gain.shape, skip_gain.dtype),
                pltpu.VMEM(taps_stage, jnp.float32),
                pltpu.VMEM((channels // phases * blocks, LANES), jnp.float32),
                pltpu.VMEM(both_message, jnp.bfloat16),
                pltpu.VMEM(both_message, jnp.bfloat16),
                pltpu.VMEM(taps_message, jnp.float32),
                pltpu.VMEM((2, depth, 2 * LANES), jnp.bfloat16),
                pltpu.VMEM((2, depth, 2 * LANES), jnp.bfloat16),
                pltpu.VMEM((4, pad + n * blocks, LANES), jnp.float32),
                pltpu.VMEM((4, pad + n * blocks, LANES), jnp.float32),
                pltpu.VMEM((4, 2, 8 + n * blocks, LANES), jnp.float32),
                pltpu.VMEM(message, jnp.bfloat16),
                pltpu.VMEM(message, jnp.bfloat16),
                pltpu.VMEM((channels * blocks, LANES), jnp.float32),
                pltpu.VMEM((blocks, LANES), jnp.float32),
                pltpu.VMEM((m, blocks, LANES), jnp.float32),
                pltpu.SemaphoreType.DMA((5, phases)),
                pltpu.SemaphoreType.DMA((2, cl // returns, n)),
                pltpu.SemaphoreType.DMA((2, cl // returns, n)),
                pltpu.SemaphoreType.DMA((2, cl // returns)),
                pltpu.SemaphoreType.DMA((m,)),
                pltpu.SemaphoreType.DMA((m,)),
                pltpu.VMEM((channels * blocks, LANES), jnp.float32),
            ],
            compiler_params=pltpu.CompilerParams(
                collective_id=0, has_side_effects=True, vmem_limit_bytes=32 * 1024 * 1024
            ),
        )(*(pltpu.with_memory_space_constraint(x, pltpu.HBM) for x in (gate_in, value_in, out_gate, taps, skip_gain)))
        return pl.pallas_call(
            functools.partial(finish, blocks, channels, channels * m),
            out_shape=jax.ShapeDtypeStruct((tokens, channels), jnp.bfloat16),
            in_specs=[pl.BlockSpec(memory_space=pltpu.VMEM)] * 2,
            out_specs=pl.BlockSpec(memory_space=pltpu.HBM),
            scratch_shapes=[
                pltpu.VMEM((tokens, channels), jnp.bfloat16),
                pltpu.SemaphoreType.DMA((blocks,)),
            ],
            compiler_params=pltpu.CompilerParams(vmem_limit_bytes=8 * 1024 * 1024),
        )(mixed, sums)

    return jax.shard_map(
        local,
        mesh=mesh,
        in_specs=(P("seq", "mp"), P("seq", "mp"), P("seq", "mp"), P("seq", "mp"), P("mp")),
        out_specs=P("seq", "mp"),
        check_vma=False,
    )
```
